512 devices in a mesh: oct: 8 (over x, z_lo), space: 64 (over z_hi, y, core).
Axes of the slice: x: 4, y: 8, z: 8 (z_hi: 4, z_lo: 2; z = z_hi * 2 + z_lo), core: 2. Of those that a mesh axis runs over, the one named last changes fastest.
Arguments:
- distribution: float32 [1000, 384, 128], P('oct', 'space'), may hold values from 0.05 to 1
- collision_scale: float32 [1, 384, 128], P(None, 'space'), may hold values from 0.4 to 2.5
Outputs:
- advanced: float32 [1000, 384, 128], P('oct', 'space')
The draws below stay inside these ranges and needn't reach their ends.
All inputs are finite; a program needn't handle non-finite values.
Results may differ from the reference program's by a relative error of at most 0.0003.
Values sent between devices are 32-bit elements; how exact they have to be, the bound alone decides.
A program may use at most 64 MiB of HBM per device.

```python
import math
import jax
import jax.numpy as jnp
from jax import lax

NV = 10
NZ = 16
STEPS = 3
VEL = 1000
NX = 384
PLANE = 128


def block_levels(own_key, extent, pieces, low, largest):
    gain = 1.0
    for dim, blocks in pieces:
        draws = jax.random.uniform(jax.random.fold_in(jax.random.fold_in(own_key, 6), dim), (blocks,), jnp.float32, low / len(pieces), largest / len(pieces))
        gain = gain * jnp.repeat(jnp.exp(draws), extent[dim] // blocks).reshape((-1,) + (1,) * (len(extent) - 1 - dim))
    return gain


def setup_inputs(seed: int = 0) -> dict:
    key_of = jax.random.split(jax.random.key(seed), 3)
    return {
        "distribution": jnp.clip(jnp.exp(math.log(1.0) - 2.9957323 * jax.random.uniform(key_of[0], (VEL, NX, PLANE), jnp.float32) ** block_levels(key_of[0], (VEL, NX, PLANE), ((0, 8), (1, 64)), -0.2, 0.2)), 0.05, 1.0),
        "collision_scale": jnp.clip(jnp.exp(math.log(2.5) - 1.8325814 * jax.random.uniform(key_of[1], (1, NX, PLANE), jnp.float32) ** block_levels(key_of[1], (1, NX, PLANE), ((1, 64),), -0.2, 0.2)), 0.4, 2.5),
    }


vel_bound = 4.0
courant = 0.08
time_step = 0.08
base_rate = 0.25
visc_index = 0.81
limiter_eps = 0.01


def velocity_parts(vel_index):
    half_count = NV // 2
    per_octant = half_count ** 3
    octant = vel_index // per_octant
    within = vel_index % per_octant
    spacing = 2.0 * vel_bound / NV
    sign_x = 1.0 - 2.0 * ((octant // 4) % 2).astype(jnp.float32)
    sign_y = 1.0 - 2.0 * ((octant // 2) % 2).astype(jnp.float32)
    sign_z = 1.0 - 2.0 * (octant % 2).astype(jnp.float32)
    vel_x = sign_x * ((within // (half_count * half_count)).astype(jnp.float32) + 0.5) * spacing
    vel_y = sign_y * (((within // half_count) % half_count).astype(jnp.float32) + 0.5) * spacing
    vel_z = sign_z * ((within % half_count).astype(jnp.float32) + 0.5) * spacing
    return vel_x, vel_y, vel_z


def moment_weights(vel_x, vel_y, vel_z):
    spacing = 2.0 * vel_bound / NV
    quad = spacing ** 3 * (2.0 * math.pi) ** -1.5
    rows = [jnp.ones_like(vel_x), vel_x, vel_y, vel_z, vel_x * vel_x + vel_y * vel_y + vel_z * vel_z]
    return quad * jnp.stack(rows)


def limited(left, right):
    return left * right * (left + right) / (left * left + right * right + limiter_eps)


def divergence_periodic(field, velocity, forward, backward):
    field_next = forward(field)
    slope = limited(field - backward(field), field_next - field)
    flux = jnp.maximum(velocity, 0.0) * (field + 0.5 * slope) + jnp.minimum(velocity, 0.0) * (field_next - 0.5 * forward(slope))
    return flux - backward(flux)


def y_forward(field):
    return jnp.roll(field, -NZ, axis=-1)


def y_backward(field):
    return jnp.roll(field, NZ, axis=-1)


def z_forward(field):
    z_place = lax.iota(jnp.int32, field.shape[-1]) % NZ
    return jnp.where(z_place == NZ - 1, jnp.roll(field, NZ - 1, axis=-1), jnp.roll(field, -1, axis=-1))


def z_backward(field):
    z_place = lax.iota(jnp.int32, field.shape[-1]) % NZ
    return jnp.where(z_place == 0, jnp.roll(field, 1 - NZ, axis=-1), jnp.roll(field, 1, axis=-1))


def x_forward(field):
    return jnp.roll(field, -1, axis=1)


def x_backward(field):
    return jnp.roll(field, 1, axis=1)


def relax(field, moments, rate_scale, vel_x, vel_y, vel_z):
    moments = moments.reshape(5, 1, field.shape[1], field.shape[2])
    density = moments[0]
    flow_x = moments[1] / density
    flow_y = moments[2] / density
    flow_z = moments[3] / density
    temper = (moments[4] / density - (flow_x * flow_x + flow_y * flow_y + flow_z * flow_z)) / 3.0
    rate = base_rate * rate_scale * density * temper ** (1.0 - visc_index)
    square = (vel_x - flow_x) ** 2 + (vel_y - flow_y) ** 2 + (vel_z - flow_z) ** 2
    equil = density * temper ** (-1.5) * jnp.exp(-square / (2.0 * temper))
    return time_step * rate * (equil - field)


def reference(distribution, collision_scale):
    groups = 8
    per_group = VEL // groups
    weights = moment_weights(*velocity_parts(lax.iota(jnp.int32, VEL)))
    field = distribution
    for step_id in range(STEPS):
        moments = jnp.dot(weights, field.reshape(VEL, -1), precision=lax.Precision.HIGHEST)

        def advance_group(pair):
            piece, group_id = pair
            vel_index = group_id * per_group + lax.iota(jnp.int32, per_group)
            vel_x, vel_y, vel_z = [parts[:, None, None] for parts in velocity_parts(vel_index)]
            change = divergence_periodic(piece, vel_x, x_forward, x_backward)
            change = change + divergence_periodic(piece, vel_y, y_forward, y_backward)
            change = change + divergence_periodic(piece, vel_z, z_forward, z_backward)
            return piece - courant * change + relax(piece, moments, collision_scale, vel_x, vel_y, vel_z)

        stacked = field.reshape(groups, per_group, NX, PLANE)
        field = lax.map(advance_group, (stacked, jnp.arange(groups, dtype=jnp.int32))).reshape(VEL, NX, PLANE)
    return field
```

```python
import math

import jax
import jax.numpy as jnp
from jax import lax
from jax.experimental import pallas as pl
from jax.experimental.pallas import tpu as pltpu
from jax.sharding import PartitionSpec as P

NV = 10
NZ = 16
STEPS = 3

vel_bound = 4.0
courant = 0.08
time_step = 0.08
base_rate = 0.25
visc_index = 0.81
limiter_eps = 0.01

MESH = pl.DeviceIdType.MESH
HALF = NV // 2
LANES = 128
LAYERS = 6
SPACING = 2.0 * vel_bound / NV
QUAD = SPACING**3 * (2.0 * math.pi) ** (-1.5)
LOG2E = math.log2(math.e)


def digits(v):
    a = jnp.zeros_like(v)
    b = jnp.zeros_like(v)
    for j in range(1, HALF):
        a = a + jnp.where(v >= HALF * HALF * j, 1, 0)
    rest = v - HALF * HALF * a
    for j in range(1, HALF):
        b = b + jnp.where(rest >= HALF * j, 1, 0)
    return a, b, rest - HALF * b


def half_slope(up, mid, down):
    left = mid - up
    right = down - mid
    return (
        0.5 * left * right * (down - up) / (left * left + right * right + limiter_eps)
    )


def kernel(
    n_oct,
    n_space,
    x_ref,
    cs_ref,
    out_ref,
    field,
    trans,
    halo_up,
    halo_down,
    vmag,
    weight,
    part,
    parts_in,
    total,
    param,
    load_sem,
    hs_sem,
    hr_sem,
    ms_sem,
    mr_sem,
):
    octant = lax.axis_index("oct")
    place = lax.axis_index("space")
    neg_x = lax.div(octant, 4)
    neg_y = lax.rem(lax.div(octant, 2), 2)
    neg_z = lax.rem(octant, 2)
    n_vel = x_ref.shape[1]

    def layer(k):
        return k + neg_x * (LAYERS - 1 - 2 * k)

    loads = []
    for k in range(LAYERS):
        copy = pltpu.make_async_copy(x_ref.at[layer(k)], field.at[0, k], load_sem.at[k])
        copy.start()
        loads.append(copy)

    step_x = 1 - 2 * neg_x
    down_place = lax.rem(place + step_x + n_space, n_space)
    up_place = lax.rem(place - step_x + n_space, n_space)

    barrier = pltpu.get_barrier_semaphore()
    for j in range(1, n_oct):
        pl.semaphore_signal(
            barrier,
            inc=1,
            device_id={"oct": lax.rem(octant + j, n_oct)},
            device_id_type=MESH,
        )
    for where in (down_place, up_place):
        pl.semaphore_signal(
            barrier, inc=1, device_id={"space": where}, device_id_type=MESH
        )

    a, b, c = digits(lax.broadcasted_iota(jnp.int32, (n_vel, LANES), 0))
    for d, digit in enumerate((a, b, c)):
        vmag[d] = (digit.astype(jnp.float32) + 0.5) * SPACING
    row = lax.broadcasted_iota(jnp.int32, (32, n_vel), 0)
    a, b, c = digits(lax.broadcasted_iota(jnp.int32, (32, n_vel), 1))
    odd_x, odd_y, odd_z = 2 * a + 1, 2 * b + 1, 2 * c + 1
    square = odd_x * odd_x + odd_y * odd_y + odd_z * odd_z
    sign_x, sign_y, sign_z = 1 - 2 * neg_x, 1 - 2 * neg_y, 1 - 2 * neg_z
    moment = jnp.zeros_like(row)
    for m in range(1, 6):
        moment = moment + jnp.where(row >= LAYERS * m, 1, 0)
    value = jnp.where(moment == 0, 1, 0)
    value = jnp.where(moment == 1, sign_x * odd_x, value)
    value = jnp.where(moment == 2, sign_y * odd_y, value)
    value = jnp.where(moment == 3, sign_z * odd_z, value)
    value = jnp.where(moment == 4, square, value).astype(jnp.float32)
    which = row - LAYERS * moment
    for k in range(LAYERS):
        weight[k] = jnp.where(which == layer(k), value, 0.0).astype(jnp.bfloat16)
    for k in range(LAYERS):
        param[5, k : k + 1, :] = cs_ref[k]

    def edge(at_end):
        lane = lax.broadcasted_iota(jnp.int32, (1, 1, LANES), 2)
        return lax.rem(lane, NZ) == at_end * (NZ - 1)

    first_z = edge(neg_z)
    last_z = edge(1 - neg_z)

    def y_up(v):
        return pltpu.roll(v, NZ + neg_y * (LANES - 2 * NZ), 2)

    def y_down(v):
        return pltpu.roll(v, LANES - NZ - neg_y * (LANES - 2 * NZ), 2)

    def z_up(v):
        near = pltpu.roll(v, 1 + neg_z * (LANES - 2), 2)
        far = pltpu.roll(v, LANES - (NZ - 1) - neg_z * (LANES - 2 * (NZ - 1)), 2)
        return jnp.where(first_z, far, near)

    def z_down(v):
        near = pltpu.roll(v, LANES - 1 - neg_z * (LANES - 2), 2)
        far = pltpu.roll(v, NZ - 1 + neg_z * (LANES - 2 * (NZ - 1)), 2)
        return jnp.where(last_z, far, near)

    chunks = [
        slice(low, min(low + 32, n_vel)) for low in range(0, n_vel, 32)
    ]

    def send_halos(n):
        copies = []
        for i, (src, dst, to) in enumerate(
            (
                (field.at[n, pl.ds(LAYERS - 2, 2)], halo_up.at[n], down_place),
                (field.at[n, 0], halo_down.at[n], up_place),
            )
        ):
            copy = pltpu.make_async_remote_copy(
                src_ref=src,
                dst_ref=dst,
                send_sem=hs_sem.at[n, i],
                recv_sem=hr_sem.at[n, i],
                device_id={"space": to},
                device_id_type=MESH,
            )
            copy.start()
            copies.append(copy)
        return copies

    def send_moments(n):
        acc = jnp.zeros((32, LANES), jnp.float32)
        for k in range(LAYERS):
            rest = field[n, k]
            for piece in range(3):
                term = rest.astype(jnp.bfloat16)
                acc = acc + jnp.dot(
                    weight[k], term, preferred_element_type=jnp.float32
                )
                if piece < 2:
                    rest = rest - term.astype(jnp.float32)
        part[n] = acc
        copies = []
        for j in range(1, n_oct):
            copy = pltpu.make_async_remote_copy(
                src_ref=part.at[n],
                dst_ref=parts_in.at[n, j - 1],
                send_sem=ms_sem.at[n, j - 1],
                recv_sem=mr_sem.at[n, j - 1],
                device_id={"oct": lax.rem(octant + j, n_oct)},
                device_id_type=MESH,
            )
            copy.start()
            copies.append(copy)
        return copies

    def transport_inside(n):
        for rows in chunks:
            f = field[n, :, rows, :]
            speed_x, speed_y, speed_z = vmag[0, rows, :], vmag[1, rows, :], vmag[2, rows, :]
            g = f + half_slope(y_up(f), f, y_down(f))
            change = speed_y * (g - y_up(g))
            g = f + half_slope(z_up(f), f, z_down(f))
            change = change + speed_z * (g - z_up(g))
            t = f - courant * change
            g = f[1:-1] + half_slope(f[:-2], f[1:-1], f[2:])
            moved = (courant * speed_x) * g
            trans[0, rows, :] = t[0]
            trans[1, rows, :] = t[1] - moved[0]
            for k in range(2, LAYERS - 1):
                trans[k, rows, :] = t[k] - moved[k - 1] + moved[k - 2]
            trans[LAYERS - 1, rows, :] = t[LAYERS - 1] + moved[-1]

    def transport_border(n):
        for rows in chunks:
            speed = courant * vmag[0, rows, :]
            up2, up1 = halo_up[n, 0, rows, :], halo_up[n, 1, rows, :]
            f0, f1 = field[n, 0, rows, :], field[n, 1, rows, :]
            f4, f5 = field[n, LAYERS - 2, rows, :], field[n, LAYERS - 1, rows, :]
            down = halo_down[n, rows, :]
            into = speed * (up1 + half_slope(up2, up1, f0))
            first = speed * (f0 + half_slope(up1, f0, f1))
            last = speed * (f5 + half_slope(f4, f5, down))
            trans[0, rows, :] = trans[0, rows, :] + (into - first)
            trans[1, rows, :] = trans[1, rows, :] + first
            trans[LAYERS - 1, rows, :] = trans[LAYERS - 1, rows, :] - last

    def cell_params(n):
        acc = part[n]
        for j in range(n_oct - 1):
            acc = acc + parts_in[n, j]
        total[...] = acc
        s = [total[LAYERS * m : LAYERS * (m + 1), :] for m in range(5)]
        density = QUAD * s[0]
        inv = 1.0 / s[0]
        half = 0.5 * SPACING
        flow_x = half * s[1] * inv
        flow_y = half * s[2] * inv
        flow_z = half * s[3] * inv
        temper = (
            half * half * s[4] * inv
            - (flow_x * flow_x + flow_y * flow_y + flow_z * flow_z)
        ) / 3.0
        log_t = jnp.log(temper)
        rate = (
            (time_step * base_rate)
            * param[5, :LAYERS, :]
            * density
            * jnp.exp((1.0 - visc_index) * log_t)
        )
        param[0, :LAYERS, :] = sign_x.astype(jnp.float32) * flow_x
        param[1, :LAYERS, :] = sign_y.astype(jnp.float32) * flow_y
        param[2, :LAYERS, :] = sign_z.astype(jnp.float32) * flow_z
        param[3, :LAYERS, :] = (-0.5 * LOG2E) / temper
        param[4, :LAYERS, :] = rate * density * jnp.exp(-1.5 * log_t)
        param[6, :LAYERS, :] = rate

    def relaxed(n, k, rows):
        f = field[n, k, rows, :]
        p = [param[i, pl.ds(layer(k), 1), :] for i in range(7)]
        dx = vmag[0, rows, :] - p[0]
        dy = vmag[1, rows, :] - p[1]
        dz = vmag[2, rows, :] - p[2]
        square = dx * dx + dy * dy + dz * dz
        return trans[k, rows, :] + p[4] * jnp.exp2(square * p[3]) - p[6] * f

    for copy in loads:
        copy.wait()
    pl.semaphore_wait(barrier, n_oct + 1)

    sent = []
    halos = send_halos(0)
    for n in range(STEPS):
        moments = send_moments(n)
        sent += halos + moments
        transport_inside(n)
        for copy in halos:
            copy.wait_recv()
        transport_border(n)
        for copy in moments:
            copy.wait_recv()
        cell_params(n)
        if n < STEPS - 1:
            for k in (LAYERS - 2, LAYERS - 1, 0):
                for rows in chunks:
                    field[n + 1, k, rows, :] = relaxed(n, k, rows)
            halos = send_halos(n + 1)
            for k in range(1, LAYERS - 2):
                for rows in chunks:
                    field[n + 1, k, rows, :] = relaxed(n, k, rows)
        else:
            for k in range(LAYERS):
                for rows in chunks:
                    out_ref[layer(k), rows, :] = relaxed(n, k, rows)
    for copy in sent:
        copy.wait_send()


def solution(mesh):
    n_oct, n_space = mesh.shape["oct"], mesh.shape["space"]

    def per_device(distribution, collision_scale):
        x = jnp.transpose(distribution, (1, 0, 2))
        cs = jnp.transpose(collision_scale, (1, 0, 2))
        n_layers, n_vel, lanes = x.shape
        f32 = jnp.float32
        dma = pltpu.SemaphoreType.DMA

        def body(*refs):
            kernel(n_oct, n_space, *refs)

        out = pl.pallas_call(
            body,
            out_shape=jax.ShapeDtypeStruct(x.shape, f32),
            in_specs=[
                pl.BlockSpec(memory_space=pl.ANY),
                pl.BlockSpec(memory_space=pltpu.VMEM),
            ],
            out_specs=pl.BlockSpec(memory_space=pltpu.VMEM),
            scratch_shapes=[
                pltpu.VMEM((STEPS, n_layers, n_vel, lanes), f32),
                pltpu.VMEM((n_layers, n_vel, lanes), f32),
                pltpu.VMEM((STEPS, 2, n_vel, lanes), f32),
                pltpu.VMEM((STEPS, n_vel, lanes), f32),
                pltpu.VMEM((3, n_vel, lanes), f32),
                pltpu.VMEM((n_layers, 32, n_vel), jnp.bfloat16),
                pltpu.VMEM((STEPS, 32, lanes), f32),
                pltpu.VMEM((STEPS, n_oct - 1, 32, lanes), f32),
                pltpu.VMEM((32, lanes), f32),
                pltpu.VMEM((7, 8, lanes), f32),
                dma((n_layers,)),
                dma((STEPS, 2)),
                dma((STEPS, 2)),
                dma((STEPS, n_oct - 1)),
                dma((STEPS, n_oct - 1)),
            ],
            compiler_params=pltpu.CompilerParams(collective_id=0, has_side_effects=True),
        )(x, cs)
        return jnp.transpose(out, (1, 0, 2))

    return jax.shard_map(
        per_device,
        mesh=mesh,
        in_specs=(P("oct", "space", None), P(None, "space", None)),
        out_specs=P("oct", "space", None),
        check_vma=False,
    )
```

```python
import math

import jax
import jax.numpy as jnp
from jax import lax
from jax.experimental import pallas as pl
from jax.experimental.pallas import tpu as pltpu
from jax.sharding import PartitionSpec as P

NV = 10
NZ = 16
STEPS = 3

vel_bound = 4.0
courant = 0.08
time_step = 0.08
base_rate = 0.25
visc_index = 0.81
limiter_eps = 0.01

MESH = pl.DeviceIdType.MESH
HALF = NV // 2
LANES = 128
LAYERS = 6
SPACING = 2.0 * vel_bound / NV
QUAD = SPACING**3 * (2.0 * math.pi) ** (-1.5)
LOG2E = math.log2(math.e)


def digits(v):
    a = jnp.zeros_like(v)
    b = jnp.zeros_like(v)
    for j in range(1, HALF):
        a = a + jnp.where(v >= HALF * HALF * j, 1, 0)
    rest = v - HALF * HALF * a
    for j in range(1, HALF):
        b = b + jnp.where(rest >= HALF * j, 1, 0)
    return a, b, rest - HALF * b


def half_slope(up, mid, down):
    left = mid - up
    right = down - mid
    return (
        0.5 * left * right * (down - up) / (left * left + right * right + limiter_eps)
    )


def kernel(
    n_oct,
    n_space,
    x_ref,
    cs_ref,
    out_ref,
    field,
    trans,
    halo_up,
    halo_down,
    vmag,
    weight,
    part,
    parts_in,
    total,
    param,
    load_sem,
    hs_sem,
    hr_sem,
    ms_sem,
    mr_sem,
):
    octant = lax.axis_index("oct")
    place = lax.axis_index("space")
    neg_x = lax.div(octant, 4)
    neg_y = lax.rem(lax.div(octant, 2), 2)
    neg_z = lax.rem(octant, 2)
    n_vel = x_ref.shape[1]

    def layer(k):
        return k + neg_x * (LAYERS - 1 - 2 * k)

    loads = []
    for k in range(LAYERS):
        copy = pltpu.make_async_copy(x_ref.at[layer(k)], field.at[0, k], load_sem.at[k])
        copy.start()
        loads.append(copy)

    step_x = 1 - 2 * neg_x
    down_place = lax.rem(place + step_x + n_space, n_space)
    up_place = lax.rem(place - step_x + n_space, n_space)

    barrier = pltpu.get_barrier_semaphore()
    for j in range(1, n_oct):
        pl.semaphore_signal(
            barrier,
            inc=1,
            device_id={"oct": lax.rem(octant + j, n_oct)},
            device_id_type=MESH,
        )
    for where in (down_place, up_place):
        pl.semaphore_signal(
            barrier, inc=1, device_id={"space": where}, device_id_type=MESH
        )

    a, b, c = digits(lax.broadcasted_iota(jnp.int32, (n_vel, LANES), 0))
    for d, digit in enumerate((a, b, c)):
        vmag[d] = (digit.astype(jnp.float32) + 0.5) * SPACING
    row = lax.broadcasted_iota(jnp.int32, (32, n_vel), 0)
    a, b, c = digits(lax.broadcasted_iota(jnp.int32, (32, n_vel), 1))
    odd_x, odd_y, odd_z = 2 * a + 1, 2 * b + 1, 2 * c + 1
    square = odd_x * odd_x + odd_y * odd_y + odd_z * odd_z
    sign_x, sign_y, sign_z = 1 - 2 * neg_x, 1 - 2 * neg_y, 1 - 2 * neg_z
    moment = jnp.zeros_like(row)
    for m in range(1, 6):
        moment = moment + jnp.where(row >= LAYERS * m, 1, 0)
    value = jnp.where(moment == 0, 1, 0)
    value = jnp.where(moment == 1, sign_x * odd_x, value)
    value = jnp.where(moment == 2, sign_y * odd_y, value)
    value = jnp.where(moment == 3, sign_z * odd_z, value)
    value = jnp.where(moment == 4, square, value).astype(jnp.float32)
    which = row - LAYERS * moment
    for k in range(LAYERS):
        weight[k] = jnp.where(which == layer(k), value, 0.0).astype(jnp.bfloat16)
    for k in range(LAYERS):
        param[5, k : k + 1, :] = cs_ref[k]

    def edge(at_end):
        lane = lax.broadcasted_iota(jnp.int32, (1, 1, LANES), 2)
        return lax.rem(lane, NZ) == at_end * (NZ - 1)

    first_z = edge(neg_z)
    last_z = edge(1 - neg_z)

    def y_up(v):
        return pltpu.roll(v, NZ + neg_y * (LANES - 2 * NZ), 2)

    def y_down(v):
        return pltpu.roll(v, LANES - NZ - neg_y * (LANES - 2 * NZ), 2)

    def z_up(v):
        near = pltpu.roll(v, 1 + neg_z * (LANES - 2), 2)
        far = pltpu.roll(v, LANES - (NZ - 1) - neg_z * (LANES - 2 * (NZ - 1)), 2)
        return jnp.where(first_z, far, near)

    def z_down(v):
        near = pltpu.roll(v, LANES - 1 - neg_z * (LANES - 2), 2)
        far = pltpu.roll(v, NZ - 1 + neg_z * (LANES - 2 * (NZ - 1)), 2)
        return jnp.where(last_z, far, near)

    chunks = [
        slice(low, min(low + 32, n_vel)) for low in range(0, n_vel, 32)
    ]

    def send_layer(n, i):
        src, dst, to = (
            (LAYERS - 2, halo_up.at[n, 0], down_place),
            (LAYERS - 1, halo_up.at[n, 1], down_place),
            (0, halo_down.at[n], up_place),
        )[i]
        copy = pltpu.make_async_remote_copy(
            src_ref=field.at[n, src],
            dst_ref=dst,
            send_sem=hs_sem.at[n, i],
            recv_sem=hr_sem.at[n, i],
            device_id={"space": to},
            device_id_type=MESH,
        )
        copy.start()
        return copy

    def moments_of(n, layers):
        acc = jnp.zeros((32, LANES), jnp.float32)
        for k in layers:
            rest = field[n, k]
            for piece in range(3):
                term = rest.astype(jnp.bfloat16)
                acc = acc + jnp.dot(
                    weight[k], term, preferred_element_type=jnp.float32
                )
                if piece < 2:
                    rest = rest - term.astype(jnp.float32)
        return acc

    def send_moments(n, acc):
        part[n] = acc
        copies = []
        for j in range(1, n_oct):
            copy = pltpu.make_async_remote_copy(
                src_ref=part.at[n],
                dst_ref=parts_in.at[n, j - 1],
                send_sem=ms_sem.at[n, j - 1],
                recv_sem=mr_sem.at[n, j - 1],
                device_id={"oct": lax.rem(octant + j, n_oct)},
                device_id_type=MESH,
            )
            copy.start()
            copies.append(copy)
        return copies

    def transport_inside(n):
        for rows in chunks:
            f = field[n, :, rows, :]
            speed_x, speed_y, speed_z = vmag[0, rows, :], vmag[1, rows, :], vmag[2, rows, :]
            g = f + half_slope(y_up(f), f, y_down(f))
            change = speed_y * (g - y_up(g))
            g = f + half_slope(z_up(f), f, z_down(f))
            change = change + speed_z * (g - z_up(g))
            t = f - courant * change
            g = f[1:-1] + half_slope(f[:-2], f[1:-1], f[2:])
            moved = (courant * speed_x) * g
            trans[0, rows, :] = t[0]
            trans[1, rows, :] = t[1] - moved[0]
            for k in range(2, LAYERS - 1):
                trans[k, rows, :] = t[k] - moved[k - 1] + moved[k - 2]
            trans[LAYERS - 1, rows, :] = t[LAYERS - 1] + moved[-1]

    def put(n, k, rows, new):
        if n < STEPS - 1:
            field[n + 1, k, rows, :] = new
        else:
            out_ref[layer(k), rows, :] = new

    def finish_border(n):
        for rows in chunks:
            speed = courant * vmag[0, rows, :]
            up2, up1 = halo_up[n, 0, rows, :], halo_up[n, 1, rows, :]
            f0, f1 = field[n, 0, rows, :], field[n, 1, rows, :]
            f4, f5 = field[n, LAYERS - 2, rows, :], field[n, LAYERS - 1, rows, :]
            down = halo_down[n, rows, :]
            into = speed * (up1 + half_slope(up2, up1, f0))
            first = speed * (f0 + half_slope(up1, f0, f1))
            last = speed * (f5 + half_slope(f4, f5, down))
            put(n, LAYERS - 1, rows, trans[LAYERS - 1, rows, :] - last)
            put(n, 0, rows, trans[0, rows, :] + (into - first))
            put(n, 1, rows, trans[1, rows, :] + first)

    def cell_params(n):
        acc = part[n]
        for j in range(n_oct - 1):
            acc = acc + parts_in[n, j]
        total[...] = acc
        s = [total[LAYERS * m : LAYERS * (m + 1), :] for m in range(5)]
        density = QUAD * s[0]
        inv = 1.0 / s[0]
        half = 0.5 * SPACING
        flow_x = half * s[1] * inv
        flow_y = half * s[2] * inv
        flow_z = half * s[3] * inv
        temper = (
            half * half * s[4] * inv
            - (flow_x * flow_x + flow_y * flow_y + flow_z * flow_z)
        ) / 3.0
        log_t = jnp.log(temper)
        rate = (
            (time_step * base_rate)
            * param[5, :LAYERS, :]
            * density
            * jnp.exp((1.0 - visc_index) * log_t)
        )
        param[0, :LAYERS, :] = sign_x.astype(jnp.float32) * flow_x
        param[1, :LAYERS, :] = sign_y.astype(jnp.float32) * flow_y
        param[2, :LAYERS, :] = sign_z.astype(jnp.float32) * flow_z
        param[3, :LAYERS, :] = (-0.5 * LOG2E) / temper
        param[4, :LAYERS, :] = rate * density * jnp.exp(-1.5 * log_t)
        param[6, :LAYERS, :] = rate

    def relaxed(n, k, rows):
        f = field[n, k, rows, :]
        p = [param[i, pl.ds(layer(k), 1), :] for i in range(7)]
        dx = vmag[0, rows, :] - p[0]
        dy = vmag[1, rows, :] - p[1]
        dz = vmag[2, rows, :] - p[2]
        square = dx * dx + dy * dy + dz * dz
        return trans[k, rows, :] + p[4] * jnp.exp2(square * p[3]) - p[6] * f

    for copy in loads:
        copy.wait()
    pl.semaphore_wait(barrier, n_oct + 1)

    border = (0, 1, LAYERS - 1)
    inside = tuple(range(2, LAYERS - 1))
    halos = [send_layer(0, i) for i in (1, 0, 2)]
    moments = send_moments(0, moments_of(0, range(LAYERS)))
    sent = halos + moments
    for n in range(STEPS):
        more = n < STEPS - 1
        transport_inside(n)
        for copy in moments:
            copy.wait_recv()
        cell_params(n)
        early = []
        for k in reversed(inside):
            for rows in chunks:
                put(n, k, rows, relaxed(n, k, rows))
            if more and k == LAYERS - 2:
                early.append(send_layer(n + 1, 0))
        for k in border:
            for rows in chunks:
                trans[k, rows, :] = relaxed(n, k, rows)
        if more:
            acc = moments_of(n + 1, inside)
        for copy in halos:
            copy.wait_recv()
        finish_border(n)
        if more:
            halos = early + [send_layer(n + 1, i) for i in (1, 2)]
            moments = send_moments(n + 1, acc + moments_of(n + 1, border))
            sent += halos + moments
    for copy in sent:
        copy.wait_send()


def solution(mesh):
    n_oct, n_space = mesh.shape["oct"], mesh.shape["space"]

    def per_device(distribution, collision_scale):
        x = jnp.transpose(distribution, (1, 0, 2))
        cs = jnp.transpose(collision_scale, (1, 0, 2))
        n_layers, n_vel, lanes = x.shape
        f32 = jnp.float32
        dma = pltpu.SemaphoreType.DMA

        def body(*refs):
            kernel(n_oct, n_space, *refs)

        out = pl.pallas_call(
            body,
            out_shape=jax.ShapeDtypeStruct(x.shape, f32),
            in_specs=[
                pl.BlockSpec(memory_space=pltpu.HBM),
                pl.BlockSpec(memory_space=pltpu.VMEM),
            ],
            out_specs=pl.BlockSpec(memory_space=pltpu.VMEM),
            scratch_shapes=[
                pltpu.VMEM((STEPS, n_layers, n_vel, lanes), f32),
                pltpu.VMEM((n_layers, n_vel, lanes), f32),
                pltpu.VMEM((STEPS, 2, n_vel, lanes), f32),
                pltpu.VMEM((STEPS, n_vel, lanes), f32),
                pltpu.VMEM((3, n_vel, lanes), f32),
                pltpu.VMEM((n_layers, 32, n_vel), jnp.bfloat16),
                pltpu.VMEM((STEPS, 32, lanes), f32),
                pltpu.VMEM((STEPS, n_oct - 1, 32, lanes), f32),
                pltpu.VMEM((32, lanes), f32),
                pltpu.VMEM((7, 8, lanes), f32),
                dma((n_layers,)),
                dma((STEPS, 3)),
                dma((STEPS, 3)),
                dma((STEPS, n_oct - 1)),
                dma((STEPS, n_oct - 1)),
            ],
            compiler_params=pltpu.CompilerParams(
                collective_id=0, has_side_effects=True, vmem_limit_bytes=8 * 2**20
            ),
        )(x, cs)
        return jnp.transpose(out, (1, 0, 2))

    return jax.shard_map(
        per_device,
        mesh=mesh,
        in_specs=(P("oct", "space", None), P(None, "space", None)),
        out_specs=P("oct", "space", None),
        check_vma=False,
    )
```

```python
import math

import jax
import jax.numpy as jnp
from jax import lax
from jax.experimental import pallas as pl
from jax.experimental.pallas import tpu as pltpu
from jax.sharding import PartitionSpec as P

NV = 10
NZ = 16
STEPS = 3

vel_bound = 4.0
courant = 0.08
time_step = 0.08
base_rate = 0.25
visc_index = 0.81
limiter_eps = 0.01

MESH = pl.DeviceIdType.MESH
HALF = NV // 2
LANES = 128
LAYERS = 6
SPACING = 2.0 * vel_bound / NV
QUAD = SPACING**3 * (2.0 * math.pi) ** (-1.5)
LOG2E = math.log2(math.e)


def digits(v):
    a = jnp.zeros_like(v)
    b = jnp.zeros_like(v)
    for j in range(1, HALF):
        a = a + jnp.where(v >= HALF * HALF * j, 1, 0)
    rest = v - HALF * HALF * a
    for j in range(1, HALF):
        b = b + jnp.where(rest >= HALF * j, 1, 0)
    return a, b, rest - HALF * b


def half_slope(up, mid, down):
    left = mid - up
    right = down - mid
    return (
        0.5 * left * right * (down - up) / (left * left + right * right + limiter_eps)
    )


def kernel(
    n_oct,
    n_space,
    x_ref,
    cs_ref,
    out_ref,
    field,
    trans,
    halo_up,
    halo_down,
    vmag,
    weight,
    part,
    parts_in,
    total,
    param,
    scale,
    load_sem,
    hs_sem,
    hr_sem,
    ms_sem,
    mr_sem,
):
    octant = lax.axis_index("oct")
    place = lax.axis_index("space")
    neg_x = lax.div(octant, 4)
    neg_y = lax.rem(lax.div(octant, 2), 2)
    neg_z = lax.rem(octant, 2)
    n_vel = x_ref.shape[1]

    def layer(k):
        return k + neg_x * (LAYERS - 1 - 2 * k)

    loads = []
    for k in range(LAYERS):
        copy = pltpu.make_async_copy(x_ref.at[layer(k)], field.at[0, k], load_sem.at[k])
        copy.start()
        loads.append(copy)

    copy = pltpu.make_async_copy(cs_ref, scale, load_sem.at[LAYERS])
    copy.start()
    loads.append(copy)

    step_x = 1 - 2 * neg_x
    down_place = lax.rem(place + step_x + n_space, n_space)
    up_place = lax.rem(place - step_x + n_space, n_space)

    barrier = pltpu.get_barrier_semaphore()
    for j in range(1, n_oct):
        pl.semaphore_signal(
            barrier,
            inc=1,
            device_id={"oct": lax.rem(octant + j, n_oct)},
            device_id_type=MESH,
        )
    for where in (down_place, up_place):
        pl.semaphore_signal(
            barrier, inc=1, device_id={"space": where}, device_id_type=MESH
        )

    a, b, c = digits(lax.broadcasted_iota(jnp.int32, (n_vel, LANES), 0))
    for d, digit in enumerate((a, b, c)):
        vmag[d] = (digit.astype(jnp.float32) + 0.5) * SPACING
    row = lax.broadcasted_iota(jnp.int32, (32, n_vel), 0)
    a, b, c = digits(lax.broadcasted_iota(jnp.int32, (32, n_vel), 1))
    odd_x, odd_y, odd_z = 2 * a + 1, 2 * b + 1, 2 * c + 1
    square = odd_x * odd_x + odd_y * odd_y + odd_z * odd_z
    sign_x, sign_y, sign_z = 1 - 2 * neg_x, 1 - 2 * neg_y, 1 - 2 * neg_z
    moment = jnp.zeros_like(row)
    for m in range(1, 6):
        moment = moment + jnp.where(row >= LAYERS * m, 1, 0)
    value = jnp.where(moment == 0, 1, 0)
    value = jnp.where(moment == 1, sign_x * odd_x, value)
    value = jnp.where(moment == 2, sign_y * odd_y, value)
    value = jnp.where(moment == 3, sign_z * odd_z, value)
    value = jnp.where(moment == 4, square, value).astype(jnp.float32)
    which = row - LAYERS * moment
    for k in range(LAYERS):
        weight[k] = jnp.where(which == layer(k), value, 0.0).astype(jnp.bfloat16)

    def edge(at_end):
        lane = lax.broadcasted_iota(jnp.int32, (1, 1, LANES), 2)
        return lax.rem(lane, NZ) == at_end * (NZ - 1)

    first_z = edge(neg_z)
    last_z = edge(1 - neg_z)

    def y_up(v):
        return pltpu.roll(v, NZ + neg_y * (LANES - 2 * NZ), 2)

    def y_down(v):
        return pltpu.roll(v, LANES - NZ - neg_y * (LANES - 2 * NZ), 2)

    def z_up(v):
        near = pltpu.roll(v, 1 + neg_z * (LANES - 2), 2)
        far = pltpu.roll(v, LANES - (NZ - 1) - neg_z * (LANES - 2 * (NZ - 1)), 2)
        return jnp.where(first_z, far, near)

    def z_down(v):
        near = pltpu.roll(v, LANES - 1 - neg_z * (LANES - 2), 2)
        far = pltpu.roll(v, NZ - 1 + neg_z * (LANES - 2 * (NZ - 1)), 2)
        return jnp.where(last_z, far, near)

    chunks = [
        slice(low, min(low + 32, n_vel)) for low in range(0, n_vel, 32)
    ]

    def send_layer(n, i):
        src, dst, to = (
            (LAYERS - 2, halo_up.at[n, 0], down_place),
            (LAYERS - 1, halo_up.at[n, 1], down_place),
            (0, halo_down.at[n], up_place),
        )[i]
        copy = pltpu.make_async_remote_copy(
            src_ref=field.at[n, src],
            dst_ref=dst,
            send_sem=hs_sem.at[n, i],
            recv_sem=hr_sem.at[n, i],
            device_id={"space": to},
            device_id_type=MESH,
        )
        copy.start()
        return copy

    def moments_of(n, layers):
        acc = jnp.zeros((32, LANES), jnp.float32)
        for k in layers:
            rest = field[n, k]
            for piece in range(3):
                term = rest.astype(jnp.bfloat16)
                acc = acc + jnp.dot(
                    weight[k], term, preferred_element_type=jnp.float32
                )
                if piece < 2:
                    rest = rest - term.astype(jnp.float32)
        return acc

    def send_moments(n, acc):
        part[n] = acc
        copies = []
        for j in range(1, n_oct):
            copy = pltpu.make_async_remote_copy(
                src_ref=part.at[n],
                dst_ref=parts_in.at[n, j - 1],
                send_sem=ms_sem.at[n, j - 1],
                recv_sem=mr_sem.at[n, j - 1],
                device_id={"oct": lax.rem(octant + j, n_oct)},
                device_id_type=MESH,
            )
            copy.start()
            copies.append(copy)
        return copies

    def transport_inside(n):
        for rows in chunks:
            f = field[n, :, rows, :]
            speed_x, speed_y, speed_z = vmag[0, rows, :], vmag[1, rows, :], vmag[2, rows, :]
            g = f + half_slope(y_up(f), f, y_down(f))
            change = speed_y * (g - y_up(g))
            g = f + half_slope(z_up(f), f, z_down(f))
            change = change + speed_z * (g - z_up(g))
            t = f - courant * change
            g = f[1:-1] + half_slope(f[:-2], f[1:-1], f[2:])
            moved = (courant * speed_x) * g
            trans[0, rows, :] = t[0]
            trans[1, rows, :] = t[1] - moved[0]
            for k in range(2, LAYERS - 1):
                trans[k, rows, :] = t[k] - moved[k - 1] + moved[k - 2]
            trans[LAYERS - 1, rows, :] = t[LAYERS - 1] + moved[-1]

    def put(n, k, rows, new):
        if n < STEPS - 1:
            field[n + 1, k, rows, :] = new
        else:
            out_ref[layer(k), rows, :] = new

    def finish_border(n):
        for rows in chunks:
            speed = courant * vmag[0, rows, :]
            up2, up1 = halo_up[n, 0, rows, :], halo_up[n, 1, rows, :]
            f0, f1 = field[n, 0, rows, :], field[n, 1, rows, :]
            f4, f5 = field[n, LAYERS - 2, rows, :], field[n, LAYERS - 1, rows, :]
            down = halo_down[n, rows, :]
            into = speed * (up1 + half_slope(up2, up1, f0))
            first = speed * (f0 + half_slope(up1, f0, f1))
            last = speed * (f5 + half_slope(f4, f5, down))
            put(n, LAYERS - 1, rows, trans[LAYERS - 1, rows, :] - last)
            put(n, 0, rows, trans[0, rows, :] + (into - first))
            put(n, 1, rows, trans[1, rows, :] + first)

    def cell_params(n):
        acc = part[n]
        for j in range(n_oct - 1):
            acc = acc + parts_in[n, j]
        total[...] = acc
        s = [total[LAYERS * m : LAYERS * (m + 1), :] for m in range(5)]
        density = QUAD * s[0]
        inv = 1.0 / s[0]
        half = 0.5 * SPACING
        flow_x = half * s[1] * inv
        flow_y = half * s[2] * inv
        flow_z = half * s[3] * inv
        temper = (
            half * half * s[4] * inv
            - (flow_x * flow_x + flow_y * flow_y + flow_z * flow_z)
        ) / 3.0
        log_t = jnp.log(temper)
        rate = (
            (time_step * base_rate)
            * param[5, :LAYERS, :]
            * density
            * jnp.exp((1.0 - visc_index) * log_t)
        )
        param[0, :LAYERS, :] = sign_x.astype(jnp.float32) * flow_x
        param[1, :LAYERS, :] = sign_y.astype(jnp.float32) * flow_y
        param[2, :LAYERS, :] = sign_z.astype(jnp.float32) * flow_z
        param[3, :LAYERS, :] = (-0.5 * LOG2E) / temper
        param[4, :LAYERS, :] = rate * density * jnp.exp(-1.5 * log_t)
        param[6, :LAYERS, :] = rate

    def relaxed(n, k, rows):
        f = field[n, k, rows, :]
        p = [param[i, pl.ds(layer(k), 1), :] for i in range(7)]
        dx = vmag[0, rows, :] - p[0]
        dy = vmag[1, rows, :] - p[1]
        dz = vmag[2, rows, :] - p[2]
        square = dx * dx + dy * dy + dz * dz
        return trans[k, rows, :] + p[4] * jnp.exp2(square * p[3]) - p[6] * f

    for copy in loads:
        copy.wait()
    for k in range(LAYERS):
        param[5, k : k + 1, :] = scale[k]
    pl.semaphore_wait(barrier, n_oct + 1)

    border = (0, 1, LAYERS - 1)
    inside = tuple(range(2, LAYERS - 1))
    halos = [send_layer(0, i) for i in (1, 0, 2)]
    moments = send_moments(0, moments_of(0, range(LAYERS)))
    sent = halos + moments
    for n in range(STEPS):
        more = n < STEPS - 1
        transport_inside(n)
        for copy in moments:
            copy.wait_recv()
        cell_params(n)
        early = []
        for k in reversed(inside):
            for rows in chunks:
                put(n, k, rows, relaxed(n, k, rows))
            if more and k == LAYERS - 2:
                early.append(send_layer(n + 1, 0))
        for k in border:
            for rows in chunks:
                trans[k, rows, :] = relaxed(n, k, rows)
        if more:
            acc = moments_of(n + 1, inside)
        for copy in halos:
            copy.wait_recv()
        finish_border(n)
        if more:
            halos = early + [send_layer(n + 1, i) for i in (1, 2)]
            moments = send_moments(n + 1, acc + moments_of(n + 1, border))
            sent += halos + moments
    for copy in sent:
        copy.wait_send()


def solution(mesh):
    n_oct, n_space = mesh.shape["oct"], mesh.shape["space"]

    def per_device(distribution, collision_scale):
        x = jnp.transpose(distribution, (1, 0, 2))
        cs = jnp.transpose(collision_scale, (1, 0, 2))
        x = pltpu.with_memory_space_constraint(x, pltpu.HBM)
        cs = pltpu.with_memory_space_constraint(cs, pltpu.HBM)
        n_layers, n_vel, lanes = x.shape
        f32 = jnp.float32
        dma = pltpu.SemaphoreType.DMA

        def body(*refs):
            kernel(n_oct, n_space, *refs)

        out = pl.pallas_call(
            body,
            out_shape=jax.ShapeDtypeStruct(x.shape, f32),
            in_specs=[
                pl.BlockSpec(memory_space=pltpu.HBM),
                pl.BlockSpec(memory_space=pltpu.HBM),
            ],
            out_specs=pl.BlockSpec(memory_space=pltpu.VMEM),
            scratch_shapes=[
                pltpu.VMEM((STEPS, n_layers, n_vel, lanes), f32),
                pltpu.VMEM((n_layers, n_vel, lanes), f32),
                pltpu.VMEM((STEPS, 2, n_vel, lanes), f32),
                pltpu.VMEM((STEPS, n_vel, lanes), f32),
                pltpu.VMEM((3, n_vel, lanes), f32),
                pltpu.VMEM((n_layers, 32, n_vel), jnp.bfloat16),
                pltpu.VMEM((STEPS, 32, lanes), f32),
                pltpu.VMEM((STEPS, n_oct - 1, 32, lanes), f32),
                pltpu.VMEM((32, lanes), f32),
                pltpu.VMEM((7, 8, lanes), f32),
                pltpu.VMEM((n_layers, 1, lanes), f32),
                dma((n_layers + 1,)),
                dma((STEPS, 3)),
                dma((STEPS, 3)),
                dma((STEPS, n_oct - 1)),
                dma((STEPS, n_oct - 1)),
            ],
            compiler_params=pltpu.CompilerParams(
                collective_id=0, has_side_effects=True, vmem_limit_bytes=8 * 2**20
            ),
        )(x, cs)
        return jnp.transpose(out, (1, 0, 2))

    return jax.shard_map(
        per_device,
        mesh=mesh,
        in_specs=(P("oct", "space", None), P(None, "space", None)),
        out_specs=P("oct", "space", None),
        check_vma=False,
    )
```

```python
import math

import jax
import jax.numpy as jnp
from jax import lax
from jax.experimental import pallas as pl
from jax.experimental.pallas import tpu as pltpu
from jax.sharding import PartitionSpec as P

NV = 10
NZ = 16
STEPS = 3

vel_bound = 4.0
courant = 0.08
time_step = 0.08
base_rate = 0.25
visc_index = 0.81
limiter_eps = 0.01

MESH = pl.DeviceIdType.MESH
HALF = NV // 2
LANES = 128
LAYERS = 6
SPACING = 2.0 * vel_bound / NV
QUAD = SPACING**3 * (2.0 * math.pi) ** (-1.5)
LOG2E = math.log2(math.e)


def digits(v):
    a = jnp.zeros_like(v)
    b = jnp.zeros_like(v)
    for j in range(1, HALF):
        a = a + jnp.where(v >= HALF * HALF * j, 1, 0)
    rest = v - HALF * HALF * a
    for j in range(1, HALF):
        b = b + jnp.where(rest >= HALF * j, 1, 0)
    return a, b, rest - HALF * b


def half_slope(up, mid, down):
    left = mid - up
    right = down - mid
    return (
        0.5 * left * right * (down - up) / (left * left + right * right + limiter_eps)
    )


def kernel(
    n_oct,
    n_space,
    x_ref,
    cs_ref,
    out_ref,
    field,
    trans,
    wide_up,
    wide_down,
    halo_up,
    halo_down,
    vmag,
    weight,
    part,
    parts_in,
    total,
    param,
    param_up,
    param_down,
    scale_in,
    scale,
    load_sem,
    hs_sem,
    hr_sem,
    ps_sem,
    pr_sem,
    ms_sem,
    mr_sem,
):
    octant = lax.axis_index("oct")
    place = lax.axis_index("space")
    neg_x = lax.div(octant, 4)
    neg_y = lax.rem(lax.div(octant, 2), 2)
    neg_z = lax.rem(octant, 2)
    n_vel = x_ref.shape[1]

    def layer(k):
        return k + neg_x * (LAYERS - 1 - 2 * k)

    loads = []
    for k in range(LAYERS):
        copy = pltpu.make_async_copy(x_ref.at[layer(k)], field.at[0, k], load_sem.at[k])
        copy.start()
        loads.append(copy)

    copy = pltpu.make_async_copy(cs_ref, scale_in, load_sem.at[LAYERS])
    copy.start()
    loads.append(copy)

    step_x = 1 - 2 * neg_x
    down_place = lax.rem(place + step_x + n_space, n_space)
    up_place = lax.rem(place - step_x + n_space, n_space)

    barrier = pltpu.get_barrier_semaphore()
    for j in range(1, n_oct):
        pl.semaphore_signal(
            barrier,
            inc=1,
            device_id={"oct": lax.rem(octant + j, n_oct)},
            device_id_type=MESH,
        )
    for where in (down_place, up_place):
        pl.semaphore_signal(
            barrier, inc=1, device_id={"space": where}, device_id_type=MESH
        )

    a, b, c = digits(lax.broadcasted_iota(jnp.int32, (n_vel, LANES), 0))
    for d, digit in enumerate((a, b, c)):
        vmag[d] = (digit.astype(jnp.float32) + 0.5) * SPACING
    row = lax.broadcasted_iota(jnp.int32, (32, n_vel), 0)
    a, b, c = digits(lax.broadcasted_iota(jnp.int32, (32, n_vel), 1))
    odd_x, odd_y, odd_z = 2 * a + 1, 2 * b + 1, 2 * c + 1
    square = odd_x * odd_x + odd_y * odd_y + odd_z * odd_z
    sign_x, sign_y, sign_z = 1 - 2 * neg_x, 1 - 2 * neg_y, 1 - 2 * neg_z
    moment = jnp.zeros_like(row)
    for m in range(1, 6):
        moment = moment + jnp.where(row >= LAYERS * m, 1, 0)
    value = jnp.where(moment == 0, 1, 0)
    value = jnp.where(moment == 1, sign_x * odd_x, value)
    value = jnp.where(moment == 2, sign_y * odd_y, value)
    value = jnp.where(moment == 3, sign_z * odd_z, value)
    value = jnp.where(moment == 4, square, value).astype(jnp.float32)
    which = row - LAYERS * moment
    for k in range(LAYERS):
        weight[k] = jnp.where(which == layer(k), value, 0.0).astype(jnp.bfloat16)

    param[...] = jnp.zeros_like(param)

    def edge(at_end):
        lane = lax.broadcasted_iota(jnp.int32, (1, 1, LANES), 2)
        return lax.rem(lane, NZ) == at_end * (NZ - 1)

    first_z = edge(neg_z)
    last_z = edge(1 - neg_z)

    def y_up(v):
        return pltpu.roll(v, NZ + neg_y * (LANES - 2 * NZ), 2)

    def y_down(v):
        return pltpu.roll(v, LANES - NZ - neg_y * (LANES - 2 * NZ), 2)

    def z_up(v):
        near = pltpu.roll(v, 1 + neg_z * (LANES - 2), 2)
        far = pltpu.roll(v, LANES - (NZ - 1) - neg_z * (LANES - 2 * (NZ - 1)), 2)
        return jnp.where(first_z, far, near)

    def z_down(v):
        near = pltpu.roll(v, LANES - 1 - neg_z * (LANES - 2), 2)
        far = pltpu.roll(v, NZ - 1 + neg_z * (LANES - 2 * (NZ - 1)), 2)
        return jnp.where(last_z, far, near)

    chunks = [
        slice(low, min(low + 32, n_vel)) for low in range(0, n_vel, 32)
    ]

    end = LAYERS - 1
    halo_plan = (
        (field.at[0, end], wide_up.at[3], down_place),
        (field.at[0, end - 1], wide_up.at[2], down_place),
        (field.at[0, 0], wide_down.at[0], up_place),
        (field.at[0, pl.ds(end - 3, 2)], wide_up.at[pl.ds(0, 2)], down_place),
        (field.at[0, 1], wide_down.at[1], up_place),
        (field.at[2, end - 1], halo_up.at[1, 0], down_place),
        (field.at[2, end], halo_up.at[1, 1], down_place),
        (field.at[2, 0], halo_down.at[1], up_place),
    )

    def send(src, dst, to, send_sem, recv_sem):
        copy = pltpu.make_async_remote_copy(
            src_ref=src,
            dst_ref=dst,
            send_sem=send_sem,
            recv_sem=recv_sem,
            device_id={"space": to},
            device_id_type=MESH,
        )
        copy.start()
        return copy

    def send_halo(i):
        return send(*halo_plan[i], hs_sem.at[i], hr_sem.at[i])

    def send_params():
        return [
            send(param.at[0], param_up, down_place, ps_sem.at[0], pr_sem.at[0]),
            send(param.at[0], param_down, up_place, ps_sem.at[1], pr_sem.at[1]),
        ]

    def halo(n, rows):
        if n == 0:
            return wide_up[2, rows, :], wide_up[3, rows, :], wide_down[0, rows, :]
        return (
            halo_up[n - 1, 0, rows, :],
            halo_up[n - 1, 1, rows, :],
            halo_down[n - 1, rows, :],
        )

    def moments_of(n, layers):
        acc = jnp.zeros((32, LANES), jnp.float32)
        for k in layers:
            rest = field[n, k]
            for piece in range(3):
                term = rest.astype(jnp.bfloat16)
                acc = acc + jnp.dot(
                    weight[k], term, preferred_element_type=jnp.float32
                )
                if piece < 2:
                    rest = rest - term.astype(jnp.float32)
        return acc

    def send_moments(n, acc):
        part[n] = acc
        copies = []
        for j in range(1, n_oct):
            copy = pltpu.make_async_remote_copy(
                src_ref=part.at[n],
                dst_ref=parts_in.at[n, j - 1],
                send_sem=ms_sem.at[n, j - 1],
                recv_sem=mr_sem.at[n, j - 1],
                device_id={"oct": lax.rem(octant + j, n_oct)},
                device_id_type=MESH,
            )
            copy.start()
            copies.append(copy)
        return copies

    def moved_yz(f, speed_y, speed_z):
        g = f + half_slope(y_up(f), f, y_down(f))
        change = speed_y * (g - y_up(g))
        g = f + half_slope(z_up(f), f, z_down(f))
        change = change + speed_z * (g - z_up(g))
        return f - courant * change

    def transport_inside(n):
        for rows in chunks:
            f = field[n, :, rows, :]
            speed_x, speed_y, speed_z = vmag[0, rows, :], vmag[1, rows, :], vmag[2, rows, :]
            t = moved_yz(f, speed_y, speed_z)
            g = f[1:-1] + half_slope(f[:-2], f[1:-1], f[2:])
            moved = (courant * speed_x) * g
            trans[0, rows, :] = t[0]
            trans[1, rows, :] = t[1] - moved[0]
            for k in range(2, LAYERS - 1):
                trans[k, rows, :] = t[k] - moved[k - 1] + moved[k - 2]
            trans[LAYERS - 1, rows, :] = t[LAYERS - 1] + moved[-1]

    def put(n, k, rows, new):
        if n < STEPS - 1:
            field[n + 1, k, rows, :] = new
        else:
            out_ref[layer(k), rows, :] = new

    def finish_border(n):
        for rows in chunks:
            speed = courant * vmag[0, rows, :]
            up2, up1, down = halo(n, rows)
            f0, f1 = field[n, 0, rows, :], field[n, 1, rows, :]
            f4, f5 = field[n, LAYERS - 2, rows, :], field[n, LAYERS - 1, rows, :]
            into = speed * (up1 + half_slope(up2, up1, f0))
            first = speed * (f0 + half_slope(up1, f0, f1))
            last = speed * (f5 + half_slope(f4, f5, down))
            put(n, LAYERS - 1, rows, trans[LAYERS - 1, rows, :] - last)
            put(n, 0, rows, trans[0, rows, :] + (into - first))
            put(n, 1, rows, trans[1, rows, :] + first)

    def cell_params(n):
        acc = part[n]
        for j in range(n_oct - 1):
            acc = acc + parts_in[n, j]
        total[...] = acc
        s = [total[LAYERS * m : LAYERS * (m + 1), :] for m in range(5)]
        density = QUAD * s[0]
        inv = 1.0 / s[0]
        half = 0.5 * SPACING
        flow_x = half * s[1] * inv
        flow_y = half * s[2] * inv
        flow_z = half * s[3] * inv
        temper = (
            half * half * s[4] * inv
            - (flow_x * flow_x + flow_y * flow_y + flow_z * flow_z)
        ) / 3.0
        log_t = jnp.log(temper)
        rate = (
            (time_step * base_rate)
            * scale[:LAYERS, :]
            * density
            * jnp.exp((1.0 - visc_index) * log_t)
        )
        param[n, 0, :LAYERS, :] = sign_x.astype(jnp.float32) * flow_x
        param[n, 1, :LAYERS, :] = sign_y.astype(jnp.float32) * flow_y
        param[n, 2, :LAYERS, :] = sign_z.astype(jnp.float32) * flow_z
        param[n, 3, :LAYERS, :] = (-0.5 * LOG2E) / temper
        param[n, 4, :LAYERS, :] = rate * density * jnp.exp(-1.5 * log_t)
        param[n, 5, :LAYERS, :] = rate

    def collided(f, moved, cells, k, rows):
        p = [cells[i, pl.ds(layer(k), 1), :] for i in range(6)]
        dx = vmag[0, rows, :] - p[0]
        dy = vmag[1, rows, :] - p[1]
        dz = vmag[2, rows, :] - p[2]
        square = dx * dx + dy * dy + dz * dz
        return moved + p[4] * jnp.exp2(square * p[3]) - p[5] * f

    def relaxed(n, k, rows):
        return collided(
            field[n, k, rows, :], trans[k, rows, :], param.at[n], k, rows
        )

    def ghost_layers():
        for rows in chunks:
            speed = courant * vmag[0, rows, :]
            up = [wide_up[i, rows, :] for i in range(4)]
            first = field[0, 0, rows, :]
            near = [field[0, end - 1, rows, :], field[0, end, rows, :]]
            down = [wide_down[i, rows, :] for i in range(2)]
            t = moved_yz(
                jnp.stack([up[2], up[3], down[0]]), vmag[1, rows, :], vmag[2, rows, :]
            )
            g3 = up[1] + half_slope(up[0], up[1], up[2])
            g2 = up[2] + half_slope(up[1], up[2], up[3])
            g1 = up[3] + half_slope(up[2], up[3], first)
            g5 = near[1] + half_slope(near[0], near[1], down[0])
            g6 = down[0] + half_slope(near[1], down[0], down[1])
            moved = (t[0] - speed * (g2 - g3), t[1] - speed * (g1 - g2), t[2] - speed * (g6 - g5))
            halo_up[0, 0, rows, :] = collided(up[2], moved[0], param_up, end - 1, rows)
            halo_up[0, 1, rows, :] = collided(up[3], moved[1], param_up, end, rows)
            halo_down[0, rows, :] = collided(down[0], moved[2], param_down, 0, rows)

    for copy in loads:
        copy.wait()
    for k in range(LAYERS):
        scale[k : k + 1, :] = scale_in[k]
    pl.semaphore_wait(barrier, n_oct + 1)

    border = (0, 1, end)
    inside = tuple(range(2, end))
    halos = [send_halo(i) for i in (0, 1, 2)]
    moments = send_moments(0, moments_of(0, range(LAYERS)))
    extra = [send_halo(i) for i in (3, 4)]
    sent = halos + moments + extra
    for n in range(STEPS):
        more = n < STEPS - 1
        transport_inside(n)
        if n == 1:
            for copy in extra:
                copy.wait_recv()
            ghost_layers()
        for copy in moments:
            copy.wait_recv()
        cell_params(n)
        if n == 0:
            params = send_params()
            extra += params
            sent += params
        early = []
        for k in reversed(inside):
            for rows in chunks:
                put(n, k, rows, relaxed(n, k, rows))
            if n == 1 and k == end - 1:
                early = [send_halo(5)]
        for k in border:
            for rows in chunks:
                trans[k, rows, :] = relaxed(n, k, rows)
        if more:
            acc = moments_of(n + 1, inside)
        for copy in halos:
            copy.wait_recv()
        finish_border(n)
        halos = early
        if n == 1:
            halos = early + [send_halo(6), send_halo(7)]
        if more:
            moments = send_moments(n + 1, acc + moments_of(n + 1, border))
            sent += halos + moments
    for copy in sent:
        copy.wait_send()


def solution(mesh):
    n_oct, n_space = mesh.shape["oct"], mesh.shape["space"]

    def per_device(distribution, collision_scale):
        x = jnp.transpose(distribution, (1, 0, 2))
        cs = jnp.transpose(collision_scale, (1, 0, 2))
        x = pltpu.with_memory_space_constraint(x, pltpu.HBM)
        cs = pltpu.with_memory_space_constraint(cs, pltpu.HBM)
        n_layers, n_vel, lanes = x.shape
        f32 = jnp.float32
        dma = pltpu.SemaphoreType.DMA

        def body(*refs):
            kernel(n_oct, n_space, *refs)

        out = pl.pallas_call(
            body,
            out_shape=jax.ShapeDtypeStruct(x.shape, f32),
            in_specs=[
                pl.BlockSpec(memory_space=pltpu.HBM),
                pl.BlockSpec(memory_space=pltpu.HBM),
            ],
            out_specs=pl.BlockSpec(memory_space=pltpu.VMEM),
            scratch_shapes=[
                pltpu.VMEM((STEPS, n_layers, n_vel, lanes), f32),
                pltpu.VMEM((n_layers, n_vel, lanes), f32),
                pltpu.VMEM((4, n_vel, lanes), f32),
                pltpu.VMEM((2, n_vel, lanes), f32),
                pltpu.VMEM((2, 2, n_vel, lanes), f32),
                pltpu.VMEM((2, n_vel, lanes), f32),
                pltpu.VMEM((3, n_vel, lanes), f32),
                pltpu.VMEM((n_layers, 32, n_vel), jnp.bfloat16),
                pltpu.VMEM((STEPS, 32, lanes), f32),
                pltpu.VMEM((STEPS, n_oct - 1, 32, lanes), f32),
                pltpu.VMEM((32, lanes), f32),
                pltpu.VMEM((STEPS, 6, 8, lanes), f32),
                pltpu.VMEM((6, 8, lanes), f32),
                pltpu.VMEM((6, 8, lanes), f32),
                pltpu.VMEM((n_layers, 1, lanes), f32),
                pltpu.VMEM((8, lanes), f32),
                dma((n_layers + 1,)),
                dma((8,)),
                dma((8,)),
                dma((2,)),
                dma((2,)),
                dma((STEPS, n_oct - 1)),
                dma((STEPS, n_oct - 1)),
            ],
            compiler_params=pltpu.CompilerParams(
                collective_id=0, has_side_effects=True, vmem_limit_bytes=8 * 2**20
            ),
        )(x, cs)
        return jnp.transpose(out, (1, 0, 2))

    return jax.shard_map(
        per_device,
        mesh=mesh,
        in_specs=(P("oct", "space", None), P(None, "space", None)),
        out_specs=P("oct", "space", None),
        check_vma=False,
    )
```

```python
import math

import jax
import jax.numpy as jnp
from jax import lax
from jax.experimental import pallas as pl
from jax.experimental.pallas import tpu as pltpu
from jax.sharding import PartitionSpec as P

NV = 10
NZ = 16
STEPS = 3

vel_bound = 4.0
courant = 0.08
time_step = 0.08
base_rate = 0.25
visc_index = 0.81
limiter_eps = 0.01

MESH = pl.DeviceIdType.MESH
HALF = NV // 2
LANES = 128
LAYERS = 6
SPACING = 2.0 * vel_bound / NV
QUAD = SPACING**3 * (2.0 * math.pi) ** (-1.5)
LOG2E = math.log2(math.e)


def digits(v):
    a = jnp.zeros_like(v)
    b = jnp.zeros_like(v)
    for j in range(1, HALF):
        a = a + jnp.where(v >= HALF * HALF * j, 1, 0)
    rest = v - HALF * HALF * a
    for j in range(1, HALF):
        b = b + jnp.where(rest >= HALF * j, 1, 0)
    return a, b, rest - HALF * b


def half_slope(up, mid, down):
    left = mid - up
    right = down - mid
    return (
        0.5 * left * right * (down - up) / (left * left + right * right + limiter_eps)
    )


def kernel(
    n_oct,
    n_space,
    x_ref,
    cs_ref,
    out_ref,
    field,
    trans,
    wide_up,
    wide_down,
    halo_up,
    halo_down,
    vmag,
    weight,
    part,
    parts_in,
    total,
    param,
    param_up,
    param_down,
    scale_in,
    scale,
    load_sem,
    hs_sem,
    hr_sem,
    ps_sem,
    pr_sem,
    ms_sem,
    mr_sem,
):
    octant = lax.axis_index("oct")
    place = lax.axis_index("space")
    neg_x = lax.div(octant, 4)
    neg_y = lax.rem(lax.div(octant, 2), 2)
    neg_z = lax.rem(octant, 2)
    n_vel = x_ref.shape[1]

    def layer(k):
        return k + neg_x * (LAYERS - 1 - 2 * k)

    loads = []
    for k in range(LAYERS):
        copy = pltpu.make_async_copy(x_ref.at[layer(k)], field.at[0, k], load_sem.at[k])
        copy.start()
        loads.append(copy)

    copy = pltpu.make_async_copy(cs_ref, scale_in, load_sem.at[LAYERS])
    copy.start()
    loads.append(copy)

    step_x = 1 - 2 * neg_x
    down_place = lax.rem(place + step_x + n_space, n_space)
    up_place = lax.rem(place - step_x + n_space, n_space)

    barrier = pltpu.get_barrier_semaphore()
    for j in range(1, n_oct):
        pl.semaphore_signal(
            barrier,
            inc=1,
            device_id={"oct": lax.rem(octant + j, n_oct)},
            device_id_type=MESH,
        )
    for where in (down_place, up_place):
        pl.semaphore_signal(
            barrier, inc=1, device_id={"space": where}, device_id_type=MESH
        )

    a, b, c = digits(lax.broadcasted_iota(jnp.int32, (n_vel, LANES), 0))
    for d, digit in enumerate((a, b, c)):
        vmag[d] = (digit.astype(jnp.float32) + 0.5) * SPACING
    row = lax.broadcasted_iota(jnp.int32, (32, n_vel), 0)
    a, b, c = digits(lax.broadcasted_iota(jnp.int32, (32, n_vel), 1))
    odd_x, odd_y, odd_z = 2 * a + 1, 2 * b + 1, 2 * c + 1
    square = odd_x * odd_x + odd_y * odd_y + odd_z * odd_z
    sign_x, sign_y, sign_z = 1 - 2 * neg_x, 1 - 2 * neg_y, 1 - 2 * neg_z
    moment = jnp.zeros_like(row)
    for m in range(1, 6):
        moment = moment + jnp.where(row >= LAYERS * m, 1, 0)
    value = jnp.where(moment == 0, 1, 0)
    value = jnp.where(moment == 1, sign_x * odd_x, value)
    value = jnp.where(moment == 2, sign_y * odd_y, value)
    value = jnp.where(moment == 3, sign_z * odd_z, value)
    value = jnp.where(moment == 4, square, value).astype(jnp.float32)
    which = row - LAYERS * moment
    for k in range(LAYERS):
        weight[k] = jnp.where(which == layer(k), value, 0.0).astype(jnp.bfloat16)

    param[...] = jnp.zeros_like(param)

    def edge(at_end):
        lane = lax.broadcasted_iota(jnp.int32, (1, 1, LANES), 2)
        return lax.rem(lane, NZ) == at_end * (NZ - 1)

    first_z = edge(neg_z)
    last_z = edge(1 - neg_z)

    def y_up(v):
        return pltpu.roll(v, NZ + neg_y * (LANES - 2 * NZ), 2)

    def y_down(v):
        return pltpu.roll(v, LANES - NZ - neg_y * (LANES - 2 * NZ), 2)

    def z_up(v):
        near = pltpu.roll(v, 1 + neg_z * (LANES - 2), 2)
        far = pltpu.roll(v, LANES - (NZ - 1) - neg_z * (LANES - 2 * (NZ - 1)), 2)
        return jnp.where(first_z, far, near)

    def z_down(v):
        near = pltpu.roll(v, LANES - 1 - neg_z * (LANES - 2), 2)
        far = pltpu.roll(v, NZ - 1 + neg_z * (LANES - 2 * (NZ - 1)), 2)
        return jnp.where(last_z, far, near)

    chunks = [
        slice(low, min(low + 32, n_vel)) for low in range(0, n_vel, 32)
    ]

    end = LAYERS - 1
    halo_plan = (
        (field.at[0, end], wide_up.at[3], down_place),
        (field.at[0, end - 1], wide_up.at[2], down_place),
        (field.at[0, 0], wide_down.at[0], up_place),
        (field.at[0, pl.ds(end - 3, 2)], wide_up.at[pl.ds(0, 2)], down_place),
        (field.at[0, 1], wide_down.at[1], up_place),
        (field.at[2, end - 1], halo_up.at[1, 0], down_place),
        (field.at[2, end], halo_up.at[1, 1], down_place),
        (field.at[2, 0], halo_down.at[1], up_place),
    )

    def send(src, dst, to, send_sem, recv_sem):
        copy = pltpu.make_async_remote_copy(
            src_ref=src,
            dst_ref=dst,
            send_sem=send_sem,
            recv_sem=recv_sem,
            device_id={"space": to},
            device_id_type=MESH,
        )
        copy.start()
        return copy

    def send_halo(i):
        return send(*halo_plan[i], hs_sem.at[i], hr_sem.at[i])

    def send_params():
        return [
            send(param.at[0], param_up, down_place, ps_sem.at[0], pr_sem.at[0]),
            send(param.at[0], param_down, up_place, ps_sem.at[1], pr_sem.at[1]),
        ]

    def halo(n, rows):
        if n == 0:
            return wide_up[2, rows, :], wide_up[3, rows, :], wide_down[0, rows, :]
        return (
            halo_up[n - 1, 0, rows, :],
            halo_up[n - 1, 1, rows, :],
            halo_down[n - 1, rows, :],
        )

    def moments_of(n, layers):
        acc = jnp.zeros((32, LANES), jnp.float32)
        for k in layers:
            rest = field[n, k]
            for piece in range(3):
                term = rest.astype(jnp.bfloat16)
                acc = acc + jnp.dot(
                    weight[k], term, preferred_element_type=jnp.float32
                )
                if piece < 2:
                    rest = rest - term.astype(jnp.float32)
        return acc

    def send_moments(n, acc):
        part[n] = acc
        copies = []
        for j in range(1, n_oct):
            copy = pltpu.make_async_remote_copy(
                src_ref=part.at[n],
                dst_ref=parts_in.at[n, j - 1],
                send_sem=ms_sem.at[n, j - 1],
                recv_sem=mr_sem.at[n, j - 1],
                device_id={"oct": lax.rem(octant + j, n_oct)},
                device_id_type=MESH,
            )
            copy.start()
            copies.append(copy)
        return copies

    def moved_yz(f, speed_y, speed_z):
        g = f + half_slope(y_up(f), f, y_down(f))
        change = speed_y * (g - y_up(g))
        g = f + half_slope(z_up(f), f, z_down(f))
        change = change + speed_z * (g - z_up(g))
        return f - courant * change

    def transport_inside(n):
        for rows in chunks:
            f = field[n, :, rows, :]
            speed_x, speed_y, speed_z = vmag[0, rows, :], vmag[1, rows, :], vmag[2, rows, :]
            t = moved_yz(f, speed_y, speed_z)
            g = f[1:-1] + half_slope(f[:-2], f[1:-1], f[2:])
            moved = (courant * speed_x) * g
            trans[0, rows, :] = t[0]
            trans[1, rows, :] = t[1] - moved[0]
            for k in range(2, LAYERS - 1):
                trans[k, rows, :] = t[k] - moved[k - 1] + moved[k - 2]
            trans[LAYERS - 1, rows, :] = t[LAYERS - 1] + moved[-1]

    def put(n, k, rows, new):
        if n < STEPS - 1:
            field[n + 1, k, rows, :] = new
        else:
            out_ref[layer(k), rows, :] = new

    def finish_border(n):
        for rows in chunks:
            speed = courant * vmag[0, rows, :]
            up2, up1, down = halo(n, rows)
            f0, f1 = field[n, 0, rows, :], field[n, 1, rows, :]
            f4, f5 = field[n, LAYERS - 2, rows, :], field[n, LAYERS - 1, rows, :]
            into = speed * (up1 + half_slope(up2, up1, f0))
            first = speed * (f0 + half_slope(up1, f0, f1))
            last = speed * (f5 + half_slope(f4, f5, down))
            put(n, LAYERS - 1, rows, trans[LAYERS - 1, rows, :] - last)
            put(n, 0, rows, trans[0, rows, :] + (into - first))
            put(n, 1, rows, trans[1, rows, :] + first)

    def cell_params(n):
        acc = part[n]
        for j in range(n_oct - 1):
            acc = acc + parts_in[n, j]
        total[...] = acc
        s = [total[LAYERS * m : LAYERS * (m + 1), :] for m in range(5)]
        density = QUAD * s[0]
        inv = 1.0 / s[0]
        half = 0.5 * SPACING
        flow_x = half * s[1] * inv
        flow_y = half * s[2] * inv
        flow_z = half * s[3] * inv
        temper = (
            half * half * s[4] * inv
            - (flow_x * flow_x + flow_y * flow_y + flow_z * flow_z)
        ) / 3.0
        log_t = jnp.log(temper)
        rate = (
            (time_step * base_rate)
            * scale[:LAYERS, :]
            * density
            * jnp.exp((1.0 - visc_index) * log_t)
        )
        param[n, 0, :LAYERS, :] = sign_x.astype(jnp.float32) * flow_x
        param[n, 1, :LAYERS, :] = sign_y.astype(jnp.float32) * flow_y
        param[n, 2, :LAYERS, :] = sign_z.astype(jnp.float32) * flow_z
        param[n, 3, :LAYERS, :] = (-0.5 * LOG2E) / temper
        param[n, 4, :LAYERS, :] = rate * density * jnp.exp(-1.5 * log_t)
        param[n, 5, :LAYERS, :] = rate

    def collided(f, moved, cells, k, rows):
        p = [cells[i, pl.ds(layer(k), 1), :] for i in range(6)]
        dx = vmag[0, rows, :] - p[0]
        dy = vmag[1, rows, :] - p[1]
        dz = vmag[2, rows, :] - p[2]
        square = dx * dx + dy * dy + dz * dz
        return moved + p[4] * jnp.exp2(square * p[3]) - p[5] * f

    def relaxed(n, k, rows):
        return collided(
            field[n, k, rows, :], trans[k, rows, :], param.at[n], k, rows
        )

    def ghost_layers():
        for rows in chunks:
            speed = courant * vmag[0, rows, :]
            up = [wide_up[i, rows, :] for i in range(4)]
            first = field[0, 0, rows, :]
            near = [field[0, end - 1, rows, :], field[0, end, rows, :]]
            down = [wide_down[i, rows, :] for i in range(2)]
            t = moved_yz(
                jnp.stack([up[2], up[3], down[0]]), vmag[1, rows, :], vmag[2, rows, :]
            )
            g3 = up[1] + half_slope(up[0], up[1], up[2])
            g2 = up[2] + half_slope(up[1], up[2], up[3])
            g1 = up[3] + half_slope(up[2], up[3], first)
            g5 = near[1] + half_slope(near[0], near[1], down[0])
            g6 = down[0] + half_slope(near[1], down[0], down[1])
            moved = (t[0] - speed * (g2 - g3), t[1] - speed * (g1 - g2), t[2] - speed * (g6 - g5))
            halo_up[0, 0, rows, :] = collided(up[2], moved[0], param_up, end - 1, rows)
            halo_up[0, 1, rows, :] = collided(up[3], moved[1], param_up, end, rows)
            halo_down[0, rows, :] = collided(down[0], moved[2], param_down, 0, rows)

    for copy in loads:
        copy.wait()
    for k in range(LAYERS):
        scale[k : k + 1, :] = scale_in[k]
    pl.semaphore_wait(barrier, n_oct + 1)

    border = (0, 1, end)
    inside = tuple(range(2, end))
    halos = [send_halo(i) for i in (0, 1, 2)]
    moments = send_moments(0, moments_of(0, range(LAYERS)))
    sent = halos + moments
    for n in range(STEPS):
        more = n < STEPS - 1
        transport_inside(n)
        if n == 0:
            extra = [send_halo(i) for i in (3, 4)]
            sent += extra
        if n == 1:
            for copy in extra:
                copy.wait_recv()
            ghost_layers()
        for copy in moments:
            copy.wait_recv()
        cell_params(n)
        if n == 0:
            params = send_params()
            extra += params
            sent += params
        early = []
        for k in reversed(inside):
            for rows in chunks:
                put(n, k, rows, relaxed(n, k, rows))
            if n == 1 and k == end - 1:
                early = [send_halo(5)]
        for k in border:
            for rows in chunks:
                trans[k, rows, :] = relaxed(n, k, rows)
        if more:
            acc = moments_of(n + 1, inside)
        for copy in halos:
            copy.wait_recv()
        finish_border(n)
        halos = early
        if n == 1:
            halos = early + [send_halo(6), send_halo(7)]
        if more:
            moments = send_moments(n + 1, acc + moments_of(n + 1, border))
            sent += halos + moments
    for copy in sent:
        copy.wait_send()


def solution(mesh):
    n_oct, n_space = mesh.shape["oct"], mesh.shape["space"]

    def per_device(distribution, collision_scale):
        x = jnp.transpose(distribution, (1, 0, 2))
        cs = jnp.transpose(collision_scale, (1, 0, 2))
        x = pltpu.with_memory_space_constraint(x, pltpu.HBM)
        cs = pltpu.with_memory_space_constraint(cs, pltpu.HBM)
        n_layers, n_vel, lanes = x.shape
        f32 = jnp.float32
        dma = pltpu.SemaphoreType.DMA

        def body(*refs):
            kernel(n_oct, n_space, *refs)

        out = pl.pallas_call(
            body,
            out_shape=jax.ShapeDtypeStruct(x.shape, f32),
            in_specs=[
                pl.BlockSpec(memory_space=pltpu.HBM),
                pl.BlockSpec(memory_space=pltpu.HBM),
            ],
            out_specs=pl.BlockSpec(memory_space=pltpu.VMEM),
            scratch_shapes=[
                pltpu.VMEM((STEPS, n_layers, n_vel, lanes), f32),
                pltpu.VMEM((n_layers, n_vel, lanes), f32),
                pltpu.VMEM((4, n_vel, lanes), f32),
                pltpu.VMEM((2, n_vel, lanes), f32),
                pltpu.VMEM((2, 2, n_vel, lanes), f32),
                pltpu.VMEM((2, n_vel, lanes), f32),
                pltpu.VMEM((3, n_vel, lanes), f32),
                pltpu.VMEM((n_layers, 32, n_vel), jnp.bfloat16),
                pltpu.VMEM((STEPS, 32, lanes), f32),
                pltpu.VMEM((STEPS, n_oct - 1, 32, lanes), f32),
                pltpu.VMEM((32, lanes), f32),
                pltpu.VMEM((STEPS, 6, 8, lanes), f32),
                pltpu.VMEM((6, 8, lanes), f32),
                pltpu.VMEM((6, 8, lanes), f32),
                pltpu.VMEM((n_layers, 1, lanes), f32),
                pltpu.VMEM((8, lanes), f32),
                dma((n_layers + 1,)),
                dma((8,)),
                dma((8,)),
                dma((2,)),
                dma((2,)),
                dma((STEPS, n_oct - 1)),
                dma((STEPS, n_oct - 1)),
            ],
            compiler_params=pltpu.CompilerParams(
                collective_id=0, has_side_effects=True, vmem_limit_bytes=8 * 2**20
            ),
        )(x, cs)
        return jnp.transpose(out, (1, 0, 2))

    return jax.shard_map(
        per_device,
        mesh=mesh,
        in_specs=(P("oct", "space", None), P(None, "space", None)),
        out_specs=P("oct", "space", None),
        check_vma=False,
    )
```

```python
import math

import jax
import jax.numpy as jnp
from jax import lax
from jax.experimental import pallas as pl
from jax.experimental.pallas import tpu as pltpu
from jax.sharding import PartitionSpec as P

NV = 10
NZ = 16
STEPS = 3

vel_bound = 4.0
courant = 0.08
time_step = 0.08
base_rate = 0.25
visc_index = 0.81
limiter_eps = 0.01

MESH = pl.DeviceIdType.MESH
HALF = NV // 2
LANES = 128
LAYERS = 6
SPACING = 2.0 * vel_bound / NV
QUAD = SPACING**3 * (2.0 * math.pi) ** (-1.5)
LOG2E = math.log2(math.e)


def digits(v):
    a = jnp.zeros_like(v)
    b = jnp.zeros_like(v)
    for j in range(1, HALF):
        a = a + jnp.where(v >= HALF * HALF * j, 1, 0)
    rest = v - HALF * HALF * a
    for j in range(1, HALF):
        b = b + jnp.where(rest >= HALF * j, 1, 0)
    return a, b, rest - HALF * b


def half_slope(up, mid, down):
    left = mid - up
    right = down - mid
    return (
        0.5 * left * right * (down - up) / (left * left + right * right + limiter_eps)
    )


def kernel(
    n_oct,
    n_space,
    x_ref,
    cs_ref,
    out_ref,
    field,
    trans,
    wide_up,
    wide_down,
    halo_up,
    halo_down,
    vmag,
    weight,
    part,
    parts_in,
    total,
    param,
    param_up,
    param_down,
    scale_in,
    scale,
    load_sem,
    hs_sem,
    hr_sem,
    ps_sem,
    pr_sem,
    ms_sem,
    mr_sem,
):
    octant = lax.axis_index("oct")
    place = lax.axis_index("space")
    neg_x = lax.div(octant, 4)
    neg_y = lax.rem(lax.div(octant, 2), 2)
    neg_z = lax.rem(octant, 2)
    n_vel = x_ref.shape[1]

    def layer(k):
        return k + neg_x * (LAYERS - 1 - 2 * k)

    loads = []
    for k in range(LAYERS):
        copy = pltpu.make_async_copy(x_ref.at[layer(k)], field.at[0, k], load_sem.at[k])
        copy.start()
        loads.append(copy)

    copy = pltpu.make_async_copy(cs_ref, scale_in, load_sem.at[LAYERS])
    copy.start()
    loads.append(copy)

    step_x = 1 - 2 * neg_x
    down_place = lax.rem(place + step_x + n_space, n_space)
    up_place = lax.rem(place - step_x + n_space, n_space)

    barrier = pltpu.get_barrier_semaphore()
    for j in range(1, n_oct):
        pl.semaphore_signal(
            barrier,
            inc=1,
            device_id={"oct": lax.rem(octant + j, n_oct)},
            device_id_type=MESH,
        )
    for where in (down_place, up_place):
        pl.semaphore_signal(
            barrier, inc=1, device_id={"space": where}, device_id_type=MESH
        )

    a, b, c = digits(lax.broadcasted_iota(jnp.int32, (n_vel, LANES), 0))
    for d, digit in enumerate((a, b, c)):
        vmag[d] = (digit.astype(jnp.float32) + 0.5) * SPACING
    row = lax.broadcasted_iota(jnp.int32, (32, n_vel), 0)
    a, b, c = digits(lax.broadcasted_iota(jnp.int32, (32, n_vel), 1))
    odd_x, odd_y, odd_z = 2 * a + 1, 2 * b + 1, 2 * c + 1
    square = odd_x * odd_x + odd_y * odd_y + odd_z * odd_z
    sign_x, sign_y, sign_z = 1 - 2 * neg_x, 1 - 2 * neg_y, 1 - 2 * neg_z
    moment = jnp.zeros_like(row)
    for m in range(1, 6):
        moment = moment + jnp.where(row >= LAYERS * m, 1, 0)
    value = jnp.where(moment == 0, 1, 0)
    value = jnp.where(moment == 1, sign_x * odd_x, value)
    value = jnp.where(moment == 2, sign_y * odd_y, value)
    value = jnp.where(moment == 3, sign_z * odd_z, value)
    value = jnp.where(moment == 4, square, value).astype(jnp.float32)
    which = row - LAYERS * moment
    for k in range(LAYERS):
        weight[k] = jnp.where(which == layer(k), value, 0.0).astype(jnp.bfloat16)

    param[...] = jnp.zeros_like(param)

    def edge(at_end):
        lane = lax.broadcasted_iota(jnp.int32, (1, 1, LANES), 2)
        return lax.rem(lane, NZ) == at_end * (NZ - 1)

    first_z = edge(neg_z)
    last_z = edge(1 - neg_z)

    def y_up(v):
        return pltpu.roll(v, NZ + neg_y * (LANES - 2 * NZ), 2)

    def y_down(v):
        return pltpu.roll(v, LANES - NZ - neg_y * (LANES - 2 * NZ), 2)

    def z_up(v):
        near = pltpu.roll(v, 1 + neg_z * (LANES - 2), 2)
        far = pltpu.roll(v, LANES - (NZ - 1) - neg_z * (LANES - 2 * (NZ - 1)), 2)
        return jnp.where(first_z, far, near)

    def z_down(v):
        near = pltpu.roll(v, LANES - 1 - neg_z * (LANES - 2), 2)
        far = pltpu.roll(v, NZ - 1 + neg_z * (LANES - 2 * (NZ - 1)), 2)
        return jnp.where(last_z, far, near)

    chunks = [
        slice(low, min(low + 32, n_vel)) for low in range(0, n_vel, 32)
    ]

    end = LAYERS - 1
    halo_plan = (
        (field.at[0, end], wide_up.at[3], down_place),
        (field.at[0, end - 1], wide_up.at[2], down_place),
        (field.at[0, 0], wide_down.at[0], up_place),
        (field.at[0, pl.ds(end - 3, 2)], wide_up.at[pl.ds(0, 2)], down_place),
        (field.at[0, 1], wide_down.at[1], up_place),
        (field.at[2, end - 1], halo_up.at[1, 0], down_place),
        (field.at[2, end], halo_up.at[1, 1], down_place),
        (field.at[2, 0], halo_down.at[1], up_place),
    )

    def send(src, dst, to, send_sem, recv_sem):
        copy = pltpu.make_async_remote_copy(
            src_ref=src,
            dst_ref=dst,
            send_sem=send_sem,
            recv_sem=recv_sem,
            device_id={"space": to},
            device_id_type=MESH,
        )
        copy.start()
        return copy

    def send_halo(i):
        return send(*halo_plan[i], hs_sem.at[i], hr_sem.at[i])

    def send_params():
        return [
            send(param.at[0], param_up, down_place, ps_sem.at[0], pr_sem.at[0]),
            send(param.at[0], param_down, up_place, ps_sem.at[1], pr_sem.at[1]),
        ]

    def halo(n, rows):
        if n == 0:
            return wide_up[2, rows, :], wide_up[3, rows, :], wide_down[0, rows, :]
        return (
            halo_up[n - 1, 0, rows, :],
            halo_up[n - 1, 1, rows, :],
            halo_down[n - 1, rows, :],
        )

    def moments_of(n, layers):
        acc = jnp.zeros((32, LANES), jnp.float32)
        for k in layers:
            rest = field[n, k]
            for piece in range(2):
                term = rest.astype(jnp.bfloat16)
                acc = acc + jnp.dot(
                    weight[k], term, preferred_element_type=jnp.float32
                )
                if piece < 1:
                    rest = rest - term.astype(jnp.float32)
        return acc

    def send_moments(n, acc):
        part[n] = acc
        copies = []
        for j in range(1, n_oct):
            copy = pltpu.make_async_remote_copy(
                src_ref=part.at[n],
                dst_ref=parts_in.at[n, j - 1],
                send_sem=ms_sem.at[n, j - 1],
                recv_sem=mr_sem.at[n, j - 1],
                device_id={"oct": lax.rem(octant + j, n_oct)},
                device_id_type=MESH,
            )
            copy.start()
            copies.append(copy)
        return copies

    def moved_yz(f, speed_y, speed_z):
        g = f + half_slope(y_up(f), f, y_down(f))
        change = speed_y * (g - y_up(g))
        g = f + half_slope(z_up(f), f, z_down(f))
        change = change + speed_z * (g - z_up(g))
        return f - courant * change

    def transport_inside(n):
        for rows in chunks:
            f = field[n, :, rows, :]
            speed_x, speed_y, speed_z = vmag[0, rows, :], vmag[1, rows, :], vmag[2, rows, :]
            t = moved_yz(f, speed_y, speed_z)
            g = f[1:-1] + half_slope(f[:-2], f[1:-1], f[2:])
            moved = (courant * speed_x) * g
            trans[0, rows, :] = t[0]
            trans[1, rows, :] = t[1] - moved[0]
            for k in range(2, LAYERS - 1):
                trans[k, rows, :] = t[k] - moved[k - 1] + moved[k - 2]
            trans[LAYERS - 1, rows, :] = t[LAYERS - 1] + moved[-1]

    def put(n, k, rows, new):
        if n < STEPS - 1:
            field[n + 1, k, rows, :] = new
        else:
            out_ref[layer(k), rows, :] = new

    def border_fluxes(n, rows):
        speed = courant * vmag[0, rows, :]
        up2, up1, down = halo(n, rows)
        f0, f1 = field[n, 0, rows, :], field[n, 1, rows, :]
        f4, f5 = field[n, LAYERS - 2, rows, :], field[n, LAYERS - 1, rows, :]
        into = speed * (up1 + half_slope(up2, up1, f0))
        first = speed * (f0 + half_slope(up1, f0, f1))
        last = speed * (f5 + half_slope(f4, f5, down))
        return into, first, last

    def transport_border(n):
        for rows in chunks:
            into, first, last = border_fluxes(n, rows)
            trans[0, rows, :] = trans[0, rows, :] + (into - first)
            trans[1, rows, :] = trans[1, rows, :] + first
            trans[LAYERS - 1, rows, :] = trans[LAYERS - 1, rows, :] - last

    def finish_border(n):
        for rows in chunks:
            into, first, last = border_fluxes(n, rows)
            put(n, LAYERS - 1, rows, trans[LAYERS - 1, rows, :] - last)
            put(n, 0, rows, trans[0, rows, :] + (into - first))
            put(n, 1, rows, trans[1, rows, :] + first)

    def cell_params(n):
        acc = part[n]
        for j in range(n_oct - 1):
            acc = acc + parts_in[n, j]
        total[...] = acc
        s = [total[LAYERS * m : LAYERS * (m + 1), :] for m in range(5)]
        density = QUAD * s[0]
        inv = 1.0 / s[0]
        half = 0.5 * SPACING
        flow_x = half * s[1] * inv
        flow_y = half * s[2] * inv
        flow_z = half * s[3] * inv
        temper = (
            half * half * s[4] * inv
            - (flow_x * flow_x + flow_y * flow_y + flow_z * flow_z)
        ) / 3.0
        log_t = jnp.log(temper)
        rate = (
            (time_step * base_rate)
            * scale[:LAYERS, :]
            * density
            * jnp.exp((1.0 - visc_index) * log_t)
        )
        param[n, 0, :LAYERS, :] = sign_x.astype(jnp.float32) * flow_x
        param[n, 1, :LAYERS, :] = sign_y.astype(jnp.float32) * flow_y
        param[n, 2, :LAYERS, :] = sign_z.astype(jnp.float32) * flow_z
        param[n, 3, :LAYERS, :] = (-0.5 * LOG2E) / temper
        param[n, 4, :LAYERS, :] = rate * density * jnp.exp(-1.5 * log_t)
        param[n, 5, :LAYERS, :] = rate

    def collided(f, moved, cells, k, rows):
        p = [cells[i, pl.ds(layer(k), 1), :] for i in range(6)]
        dx = vmag[0, rows, :] - p[0]
        dy = vmag[1, rows, :] - p[1]
        dz = vmag[2, rows, :] - p[2]
        square = dx * dx + dy * dy + dz * dz
        return moved + p[4] * jnp.exp2(square * p[3]) - p[5] * f

    def relaxed(n, k, rows):
        return collided(
            field[n, k, rows, :], trans[k, rows, :], param.at[n], k, rows
        )

    def ghost_layers():
        for rows in chunks:
            speed = courant * vmag[0, rows, :]
            up = [wide_up[i, rows, :] for i in range(4)]
            first = field[0, 0, rows, :]
            near = [field[0, end - 1, rows, :], field[0, end, rows, :]]
            down = [wide_down[i, rows, :] for i in range(2)]
            t = moved_yz(
                jnp.stack([up[2], up[3], down[0]]), vmag[1, rows, :], vmag[2, rows, :]
            )
            g3 = up[1] + half_slope(up[0], up[1], up[2])
            g2 = up[2] + half_slope(up[1], up[2], up[3])
            g1 = up[3] + half_slope(up[2], up[3], first)
            g5 = near[1] + half_slope(near[0], near[1], down[0])
            g6 = down[0] + half_slope(near[1], down[0], down[1])
            moved = (t[0] - speed * (g2 - g3), t[1] - speed * (g1 - g2), t[2] - speed * (g6 - g5))
            halo_up[0, 0, rows, :] = collided(up[2], moved[0], param_up, end - 1, rows)
            halo_up[0, 1, rows, :] = collided(up[3], moved[1], param_up, end, rows)
            halo_down[0, rows, :] = collided(down[0], moved[2], param_down, 0, rows)

    for copy in loads:
        copy.wait()
    for k in range(LAYERS):
        scale[k : k + 1, :] = scale_in[k]
    pl.semaphore_wait(barrier, n_oct + 1)

    border = (0, 1, end)
    inside = tuple(range(2, end))
    halos = [send_halo(i) for i in (0, 1, 2)]
    moments = send_moments(0, moments_of(0, range(LAYERS)))
    sent = halos + moments
    for n in range(STEPS):
        more = n < STEPS - 1
        transport_inside(n)
        if n == 0:
            extra = [send_halo(i) for i in (3, 4)]
            sent += extra
        if n == 1:
            for copy in extra:
                copy.wait_recv()
            ghost_layers()
            transport_border(n)
        for copy in moments:
            copy.wait_recv()
        cell_params(n)
        if n == 0:
            params = send_params()
            extra += params
            sent += params
        if n == 1:
            halos = []
            for k, i in ((end, 6), (end - 1, 5), (0, 7)):
                for rows in chunks:
                    put(n, k, rows, relaxed(n, k, rows))
                halos.append(send_halo(i))
            for k in range(1, end - 1):
                for rows in chunks:
                    put(n, k, rows, relaxed(n, k, rows))
            moments = send_moments(n + 1, moments_of(n + 1, range(LAYERS)))
            sent += halos + moments
            continue
        for k in inside:
            for rows in chunks:
                put(n, k, rows, relaxed(n, k, rows))
        for k in border:
            for rows in chunks:
                trans[k, rows, :] = relaxed(n, k, rows)
        if more:
            acc = moments_of(n + 1, inside)
        for copy in halos:
            copy.wait_recv()
        finish_border(n)
        if more:
            moments = send_moments(n + 1, acc + moments_of(n + 1, border))
            sent += moments
    for copy in sent:
        copy.wait_send()


def solution(mesh):
    n_oct, n_space = mesh.shape["oct"], mesh.shape["space"]

    def per_device(distribution, collision_scale):
        x = jnp.transpose(distribution, (1, 0, 2))
        cs = jnp.transpose(collision_scale, (1, 0, 2))
        x = pltpu.with_memory_space_constraint(x, pltpu.HBM)
        cs = pltpu.with_memory_space_constraint(cs, pltpu.HBM)
        n_layers, n_vel, lanes = x.shape
        f32 = jnp.float32
        dma = pltpu.SemaphoreType.DMA

        def body(*refs):
            kernel(n_oct, n_space, *refs)

        out = pl.pallas_call(
            body,
            out_shape=jax.ShapeDtypeStruct(x.shape, f32),
            in_specs=[
                pl.BlockSpec(memory_space=pltpu.HBM),
                pl.BlockSpec(memory_space=pltpu.HBM),
            ],
            out_specs=pl.BlockSpec(memory_space=pltpu.VMEM),
            scratch_shapes=[
                pltpu.VMEM((STEPS, n_layers, n_vel, lanes), f32),
                pltpu.VMEM((n_layers, n_vel, lanes), f32),
                pltpu.VMEM((4, n_vel, lanes), f32),
                pltpu.VMEM((2, n_vel, lanes), f32),
                pltpu.VMEM((2, 2, n_vel, lanes), f32),
                pltpu.VMEM((2, n_vel, lanes), f32),
                pltpu.VMEM((3, n_vel, lanes), f32),
                pltpu.VMEM((n_layers, 32, n_vel), jnp.bfloat16),
                pltpu.VMEM((STEPS, 32, lanes), f32),
                pltpu.VMEM((STEPS, n_oct - 1, 32, lanes), f32),
                pltpu.VMEM((32, lanes), f32),
                pltpu.VMEM((STEPS, 6, 8, lanes), f32),
                pltpu.VMEM((6, 8, lanes), f32),
                pltpu.VMEM((6, 8, lanes), f32),
                pltpu.VMEM((n_layers, 1, lanes), f32),
                pltpu.VMEM((8, lanes), f32),
                dma((n_layers + 1,)),
                dma((8,)),
                dma((8,)),
                dma((2,)),
                dma((2,)),
                dma((STEPS, n_oct - 1)),
                dma((STEPS, n_oct - 1)),
            ],
            compiler_params=pltpu.CompilerParams(
                collective_id=0, has_side_effects=True, vmem_limit_bytes=8 * 2**20
            ),
        )(x, cs)
        return jnp.transpose(out, (1, 0, 2))

    return jax.shard_map(
        per_device,
        mesh=mesh,
        in_specs=(P("oct", "space", None), P(None, "space", None)),
        out_specs=P("oct", "space", None),
        check_vma=False,
    )
```
